32 devices in a mesh: gz: 4 (over z), xy: 8 (over y, x, core).
Axes of the slice: x: 2, y: 2, z: 4, core: 2. Of those that a mesh axis runs over, the one named last changes fastest.
Arguments:
- volume: float32 [64, 384, 128], P('gz', 'xy'), may hold values from 0 to 1
- measured: float32 [2, 5, 80, 384], P(None, None, 'gz', 'xy'), may hold values from 0 to 1
- view_order: int32 [48], replicated, may hold values from 0 to 47, each once
Outputs:
- volume_out: float32 [64, 384, 128], P('gz', 'xy')
- residual: float32 [5, 80, 384], P(None, 'gz', 'xy')
The draws below stay inside these ranges and needn't reach their ends.
Inputs may be any that keep to these rules, and one draw needn't show every extreme that they name: `view_order`: A permutation of the numbers 0 to 47.
All inputs are finite; a program needn't handle non-finite values.
Results may differ from the reference program's by a relative error of at most 0.00078.
Values may be sent and summed in bfloat16 or wider, within the bound.
A program may use at most 64 MiB of HBM per device.

```python
import math
import jax
import jax.numpy as jnp
from jax import lax

X_DEV = 48
NY = 128
VIEWS = 5
SUBSETS = 2
ANGLES = 48
NX = 384
NZ = 64
DR = 80
DC = 384
N_XY = 8


def levels(own_key, extent, shards, smallest, top_value):
    def one(dim, parts):
        heights = jax.random.uniform(jax.random.fold_in(jax.random.fold_in(own_key, 6), dim), (parts,), jnp.float32, smallest / len(shards), top_value / len(shards))
        return jnp.repeat(jnp.exp(heights), extent[dim] // parts).reshape((-1,) + (1,) * (len(extent) - dim - 1))

    level = one(*shards[0])
    for cut in shards[1:]:
        level = level * one(*cut)
    return level


def setup_inputs(seed: int = 0) -> dict:
    seeds = jax.random.split(jax.random.key(seed), 4)
    return {
        "volume": jnp.clip(1.0 * jax.random.uniform(seeds[0], (NZ, NX, NY), jnp.float32) ** levels(seeds[0], (NZ, NX, NY), ((0, 4), (1, 8)), -0.2, 0.2), 0.0, 1.0),
        "measured": jnp.clip(1.0 * jax.random.uniform(seeds[1], (SUBSETS, VIEWS, DR, DC), jnp.float32) ** levels(seeds[1], (SUBSETS, VIEWS, DR, DC), ((2, 4), (3, 8)), -0.2, 0.2), 0.0, 1.0),
        "view_order": jax.random.permutation(seeds[2], ANGLES).astype(jnp.int32),
    }


def column_weights(view_angle, x_first, x_count, nx_all, ny_all, dc_all):
    x_coords = jnp.asarray(x_first).astype(jnp.float32) + jnp.arange(x_count, dtype=jnp.float32) - (nx_all - 1) / 2.0
    y_coords = jnp.arange(ny_all, dtype=jnp.float32) - (ny_all - 1) / 2.0
    cosine = jnp.cos(view_angle)
    sine_value = jnp.sin(view_angle)
    along_axis = x_coords[:, None] * cosine + y_coords[None, :] * sine_value
    depth_axis = y_coords[None, :] * cosine - x_coords[:, None] * sine_value
    source = 2.0 * nx_all
    position = (dc_all - 1) / 2.0 + 0.9 * (dc_all / nx_all) * along_axis * source / (source + depth_axis)
    position = position.reshape(x_count // 8, 8, ny_all // 16, 16).transpose(0, 2, 1, 3).reshape(-1, 128)
    lowest = jnp.min(position, axis=1)
    first_block = jnp.clip(jnp.floor(lowest / 64.0), 0, dc_all // 64 - 2).astype(jnp.int32)
    columns = (first_block * 64)[:, None] + jnp.arange(128, dtype=jnp.int32)[None, :]
    weights = jnp.maximum(0.0, 1.0 - jnp.abs(position[:, :, None] - columns[:, None, :].astype(position.dtype)))
    return weights.astype(jnp.bfloat16), first_block


def place_blocks(values, first_block, block_count):
    block_ids = jnp.arange(block_count, dtype=jnp.int32)
    low_onehot = (first_block[:, None] == block_ids[None, :]).astype(values.dtype)
    high_onehot = (first_block[:, None] + 1 == block_ids[None, :]).astype(values.dtype)
    result = jnp.einsum('sb,skc->kbc', low_onehot, values[:, :, :64], precision=lax.Precision.HIGHEST)
    result = result + jnp.einsum('sb,skc->kbc', high_onehot, values[:, :, 64:], precision=lax.Precision.HIGHEST)
    return result.reshape(values.shape[1], block_count * 64)


def row_weights(row_ids, slice_ids, dr_all, nz_all):
    position = (dr_all - 1) / 2.0 + 0.96 * (dr_all / nz_all) * (slice_ids.astype(jnp.float32) - (nz_all - 1) / 2.0)
    inside = ((row_ids >= 0) & (row_ids < dr_all)).astype(jnp.float32)
    hat = jnp.maximum(0.0, 1.0 - jnp.abs(position[None, :] - row_ids[:, None].astype(jnp.float32)) / 2.0)
    return hat * inside[:, None]


def reference(volume, measured, view_order):
    block_count = DC // 64
    tiled = volume.reshape(NZ, N_XY, X_DEV // 8, 8, NY // 16, 16).transpose(1, 2, 4, 0, 3, 5).reshape(N_XY, -1, NZ, 128)
    axial_weights = row_weights(jnp.arange(DR, dtype=jnp.int32), jnp.arange(NZ, dtype=jnp.int32), DR, NZ)
    slice_total = jnp.sum(axial_weights, axis=0)
    ray_rows = jnp.sum(axial_weights, axis=1)
    strip_ids = jnp.arange(N_XY, dtype=jnp.int32)
    residual = jnp.zeros((VIEWS, DR, DC), jnp.float32)
    for subset in range(SUBSETS):
        chosen = view_order[subset * VIEWS:(subset + 1) * VIEWS]
        angles = 2.0 * math.pi * chosen.astype(jnp.float32) / ANGLES

        def forward(totals, item):
            tiles, strip_index = item
            placed_sum, column_sum = totals
            tiles_rounded = lax.optimization_barrier(tiles.astype(jnp.bfloat16)).astype(jnp.float32)
            new_placed = []
            new_columns = []
            for view_index in range(VIEWS):
                weights, first_block = column_weights(angles[view_index], strip_index * X_DEV, X_DEV, NX, NY, DC)
                weights = lax.optimization_barrier(weights).astype(jnp.float32)
                column_sums = jnp.einsum('szv,svc->szc', tiles_rounded, weights, precision=lax.Precision.HIGHEST)
                new_placed.append(place_blocks(column_sums, first_block, block_count))
                new_columns.append(place_blocks(jnp.sum(weights, axis=1)[:, None, :], first_block, block_count)[0])
            return (placed_sum + jnp.stack(new_placed), column_sum + jnp.stack(new_columns)), None

        start = (jnp.zeros((VIEWS, NZ, DC), jnp.float32), jnp.zeros((VIEWS, DC), jnp.float32))
        (placed, column_total), leftover = lax.scan(forward, start, (tiled, strip_ids))
        projection = jnp.einsum('rz,vzc->vrc', axial_weights, placed, precision=lax.Precision.HIGHEST)
        ray_sums = ray_rows[None, :, None] * column_total[:, None, :]
        residual = measured[subset] - projection / jnp.maximum(ray_sums, 1.0)
        rounded = lax.optimization_barrier(residual.astype(jnp.bfloat16)).astype(jnp.float32)
        smeared = jnp.einsum('rz,vrc->vzc', axial_weights, rounded, precision=lax.Precision.HIGHEST).astype(jnp.bfloat16)
        smeared = lax.optimization_barrier(smeared).astype(jnp.float32)

        def backward(item):
            tiles, strip_index = item
            back_total = jnp.zeros(tiles.shape, jnp.float32)
            norm_total = jnp.zeros(tiles.shape, jnp.float32)
            for view_index in range(VIEWS):
                weights, first_block = column_weights(angles[view_index], strip_index * X_DEV, X_DEV, NX, NY, DC)
                weights = lax.optimization_barrier(weights).astype(jnp.float32)
                pieces = smeared[view_index].reshape(NZ, block_count, 64)
                window = jnp.concatenate((jnp.take(pieces, first_block, axis=1), jnp.take(pieces, first_block + 1, axis=1)), axis=2)
                back_total = back_total + jnp.einsum('zsc,svc->szv', window, weights, precision=lax.Precision.HIGHEST)
                norm_total = norm_total + slice_total[None, :, None] * jnp.sum(weights, axis=2)[:, None, :]
            return tiles + back_total / jnp.maximum(norm_total, 1.0)

        tiled = lax.map(backward, (tiled, strip_ids))
    volume_out = tiled.reshape(N_XY, X_DEV // 8, NY // 16, NZ, 8, 16).transpose(3, 0, 1, 4, 2, 5).reshape(NZ, NX, NY)
    return volume_out, residual
```

```python
import functools
import math

import jax
import jax.numpy as jnp
from jax import lax
from jax.experimental import pallas as pl
from jax.experimental.pallas import tpu as pltpu
from jax.sharding import PartitionSpec as P

VIEWS = 5
SUBSETS = 2
ANGLES = 48
TX = 8
TY = 16
WIN = 48
STEP = 16
LANES = 128
VROWS = 32
HI = lax.Precision.HIGHEST
MESH = pl.DeviceIdType.MESH
NT = (((1,), (1,)), ((), ()))


def hat(pos, rows):
    return jnp.maximum(0.0, 1.0 - jnp.abs(pos - rows) / 2.0)


def slice_position(z, dr_all, nz_all):
    return (dr_all - 1) / 2.0 + 0.96 * (dr_all / nz_all) * (z - (nz_all - 1) / 2.0)


def column_position(x, y, cosine, sine, nx_all, ny, dc_all):
    xc = x - (nx_all - 1) / 2.0
    yc = y - (ny - 1) / 2.0
    along = xc * cosine + yc * sine
    depth = yc * cosine - xc * sine
    source = 2.0 * nx_all
    return (dc_all - 1) / 2.0 + 0.9 * (dc_all / nx_all) * along * source / (source + depth)


def tile_swap(rows):
    lane = lax.broadcasted_iota(jnp.int32, rows[0].shape, 1)
    for bit in (1, 2, 4):
        high = ((lane // TY) & bit) != 0
        new = []
        for i in range(TX):
            if i & bit:
                new.append(jnp.where(high, rows[i], pltpu.roll(rows[i - bit], LANES - TY * bit, 1)))
            else:
                new.append(jnp.where(high, pltpu.roll(rows[i + bit], TY * bit, 1), rows[i]))
        rows = new
    return rows


def fill_positions(u_ref, geom_ref, subset, cfg):
    nx_all, ny, dc_all, x_dev = cfg
    tiles = u_ref.shape[1]
    tile = lax.broadcasted_iota(jnp.int32, (tiles, LANES), 0)
    lane = lax.broadcasted_iota(jnp.int32, (tiles, LANES), 1)
    per = ny // TY
    x = ((tile // per) * TX + lane // TY).astype(jnp.float32) + geom_ref[2 * VIEWS * SUBSETS]
    y = ((tile % per) * TY + lane % TY).astype(jnp.float32)
    for v in range(VIEWS):
        k = subset * VIEWS + v
        u_ref[v] = column_position(
            x, y, geom_ref[k], geom_ref[VIEWS * SUBSETS + k], nx_all, ny, dc_all
        )


def weights_for(u_ref, v, t, start):
    row = u_ref[v, pl.ds(t, 1), :] - start.astype(jnp.float32)
    col = lax.broadcasted_iota(jnp.int32, (WIN, LANES), 0).astype(jnp.float32)
    return jnp.maximum(0.0, 1.0 - jnp.abs(row - col)).astype(jnp.bfloat16)


def project_tile(tile, t, subset, starts_ref, u_ref, accs):
    z_dev = tile.shape[0]
    ones = jnp.where(
        lax.broadcasted_iota(jnp.int32, (z_dev, LANES), 0) == 0, 1.0, 0.0
    ).astype(jnp.bfloat16)
    a = jnp.concatenate([tile.astype(jnp.bfloat16), ones], axis=0)
    starts = [pl.multiple_of(starts_ref[subset * VIEWS + v, t], STEP) for v in range(VIEWS)]
    w = jnp.concatenate([weights_for(u_ref, v, t, starts[v]) for v in range(VIEWS)], axis=0)
    part = lax.dot_general(w, a, NT, preferred_element_type=jnp.float32)
    for v in range(VIEWS):
        where = pl.ds(starts[v], WIN)
        accs[v][where, : 2 * z_dev] += part[v * WIN : (v + 1) * WIN]


def clear(accs):
    for acc in accs:
        acc[...] = jnp.zeros_like(acc)


def combine(accs, part_ref, z_dev):
    total = jnp.zeros(part_ref.shape, jnp.float32)
    lane = lax.broadcasted_iota(jnp.int32, part_ref.shape, 1)
    for v in range(VIEWS):
        a = accs[v][...]
        s = jnp.where(lane < z_dev, a, 0.0)
        n = jnp.where(lane == z_dev, a, 0.0)
        total = total + (pltpu.roll(s, z_dev * v, 1) if v else s)
        total = total + pltpu.roll(n, z_dev * (VIEWS - 1) + v, 1)
    part_ref[...] = total


def forward_kernel(cfg, starts_ref, geom_ref, vol_ref, tiles_ref, part_ref, u_ref, *accs):
    nx_all, ny, dc_all, x_dev = cfg
    tiles, z_dev = tiles_ref.shape[:2]
    fill_positions(u_ref, geom_ref, 0, cfg)
    clear(accs)
    per = ny // TY
    for g in range(x_dev // TX):
        rows = [vol_ref[pl.ds(g * TX + i, z_dev, stride=x_dev), :] for i in range(TX)]
        rows = tile_swap(rows)
        for j in range(per):
            tiles_ref[g * per + j] = rows[j]

    @pl.loop(0, tiles)
    def _(t):
        project_tile(tiles_ref[t], t, 0, starts_ref, u_ref, accs)

    combine(accs, part_ref, z_dev)


def make_blocks(sm_ref, blk_ref, z_dev):
    k = sm_ref.shape[1]
    eye = (
        lax.broadcasted_iota(jnp.int32, (k, k), 0) == lax.broadcasted_iota(jnp.int32, (k, k), 1)
    ).astype(jnp.bfloat16)
    rows = lax.dot_general(eye, sm_ref[...], NT, preferred_element_type=jnp.float32)
    for s in range(blk_ref.shape[0]):
        cut = rows[: VIEWS * z_dev, s * STEP : s * STEP + WIN].astype(jnp.bfloat16)
        for v in range(VIEWS):
            blk_ref[s, v, :, :WIN] = cut[v * z_dev : (v + 1) * z_dev]


def back_tile(tile, t, subset, starts_ref, u_ref, blk_ref, slice_total):
    z_dev = tile.shape[0]
    ones = jnp.where(
        lax.broadcasted_iota(jnp.int32, (z_dev, WIN), 0) == 0, 1.0, 0.0
    ).astype(jnp.bfloat16)
    total = jnp.zeros((2 * z_dev, LANES), jnp.float32)
    for v in range(VIEWS):
        start = starts_ref[subset * VIEWS + v, t]
        w = weights_for(u_ref, v, t, start)
        a = jnp.concatenate([blk_ref[start // STEP, v][:, :WIN], ones], axis=0)
        total = total + jnp.dot(a, w, preferred_element_type=jnp.float32)
    norm = slice_total * total[z_dev : z_dev + 1]
    return tile + total[:z_dev] / jnp.maximum(norm, 1.0)


def slice_totals(geom_ref, z_dev, dr_all, nz_all):
    z = lax.broadcasted_iota(jnp.int32, (z_dev, LANES), 0).astype(jnp.float32)
    pos = slice_position(z + geom_ref[2 * VIEWS * SUBSETS + 1], dr_all, nz_all)
    total = jnp.zeros((z_dev, LANES), jnp.float32)
    for r in range(dr_all):
        total = total + hat(pos, float(r))
    return total


def back_kernel(cfg, rows_cfg, subset, starts_ref, geom_ref, tiles_ref, sm_ref, *rest):
    nx_all, ny, dc_all, x_dev = cfg
    dr_all, nz_all = rows_cfg
    tiles, z_dev = tiles_ref.shape[:2]
    last = subset == SUBSETS - 1
    if last:
        vol_ref, u_ref, blk_ref, new_ref = rest
    else:
        new_ref, part_ref, u_ref, blk_ref, u2_ref, *accs = rest
        fill_positions(u2_ref, geom_ref, subset + 1, cfg)
        clear(accs)
    fill_positions(u_ref, geom_ref, subset, cfg)
    make_blocks(sm_ref, blk_ref, z_dev)
    slice_total = slice_totals(geom_ref, z_dev, dr_all, nz_all)

    @pl.loop(0, tiles)
    def _(t):
        tile = back_tile(tiles_ref[t], t, subset, starts_ref, u_ref, blk_ref, slice_total)
        new_ref[t] = tile
        if not last:
            project_tile(tile, t, subset + 1, starts_ref, u2_ref, accs)

    if not last:
        combine(accs, part_ref, z_dev)
        return
    per = ny // TY
    for g in range(x_dev // TX):
        rows = tile_swap([new_ref[g * per + j] for j in range(per)])
        for i in range(TX):
            vol_ref[pl.ds(g * TX + i, z_dev, stride=x_dev), :] = rows[i]


def comm_kernel(dims, part_ref, meas_ref, sm_ref, *rest):
    n, ngz, z_dev, rows_dev, cols, margin = dims
    (res_ref, got, sums, nbr, mnbr, own, sa, ra, sb, rb, sm_sem, rm_sem, sc, rc) = rest
    nz_all, dr_all = z_dev * ngz, rows_dev * ngz
    gz, me = lax.axis_index("gz"), lax.axis_index("xy")
    peers = [lax.rem(me + k, n) for k in range(1, n)]
    sides = ((0, gz > 0, gz - 1), (1, gz < ngz - 1, gz + 1))

    barrier = pltpu.get_barrier_semaphore()
    for p in peers:
        pl.semaphore_signal(barrier, inc=1, device_id=(gz, p), device_id_type=MESH)
    for _, there, other in sides:

        @pl.when(there)
        def _():
            pl.semaphore_signal(barrier, inc=1, device_id=(other, me), device_id_type=MESH)

    near = lax.div(gz + ngz - 1, ngz) + lax.div(2 * ngz - 2 - gz, ngz)
    pl.semaphore_wait(barrier, n - 1 + near)

    first = []
    for k, p in enumerate(peers):
        copy = pltpu.make_async_remote_copy(
            src_ref=part_ref.at[pl.ds(pl.multiple_of(p * cols, 8), cols)],
            dst_ref=got.at[k],
            send_sem=sa.at[k],
            recv_sem=ra.at[k],
            device_id=(gz, p),
            device_id_type=MESH,
        )
        copy.start()
        first.append(copy)

    def side_copy(src, dst, side, other, send, recv):
        return pltpu.make_async_remote_copy(
            src_ref=src,
            dst_ref=dst.at[1 - side],
            send_sem=send.at[side],
            recv_sem=recv.at[1 - side],
            device_id=(other, me),
            device_id_type=MESH,
        )

    def side_wait(src, dst, side, other, send, recv):
        side_copy(src, dst, side, other, send, recv).wait_send()
        side_copy(src, dst, 1 - side, other, send, recv).wait_recv()

    for side, there, other in sides:

        @pl.when(there)
        def _():
            side_copy(meas_ref, mnbr, side, other, sm_sem, rm_sem).start()

    wide = 2 * LANES
    fz = gz.astype(jnp.float32)
    kk = lax.broadcasted_iota(jnp.int32, (LANES, wide), 0)
    ll = lax.broadcasted_iota(jnp.int32, (LANES, wide), 1)
    same = jnp.logical_and(kk // z_dev == ll // VROWS, kk < VIEWS * z_dev)
    ext = rows_dev + 2 * margin

    def row_of(lanes):
        rr = lanes % VROWS
        row = (rr - margin).astype(jnp.float32) + fz * rows_dev
        ok = (rr < ext) & (row >= 0) & (row < dr_all) & (lanes < VIEWS * VROWS)
        return rr, row, ok

    rr, row, ok = row_of(ll)
    keep = jnp.logical_and(same, ok)
    zz = (kk % z_dev).astype(jnp.float32)

    def slab(shift):
        z = zz + (fz + shift) * z_dev
        return jnp.where(keep, hat(slice_position(z, dr_all, nz_all), row), 0.0)

    mats = [slab(-1), slab(1), slab(0)]
    pick = (kk == VIEWS * z_dev + ll // VROWS).astype(jnp.float32)
    z_all = lax.broadcasted_iota(jnp.int32, (nz_all, wide), 0).astype(jnp.float32)
    _, row_all, _ = row_of(lax.broadcasted_iota(jnp.int32, (nz_all, wide), 1))
    ray_rows = jnp.sum(
        hat(slice_position(z_all, dr_all, nz_all), row_all), axis=0, keepdims=True
    )
    l2 = lax.broadcasted_iota(jnp.int32, (wide, LANES), 0)
    k2 = lax.broadcasted_iota(jnp.int32, (wide, LANES), 1)
    _, row2, ok2 = row_of(l2)
    keep2 = ok2 & (k2 // z_dev == l2 // VROWS) & (k2 < VIEWS * z_dev)
    z2 = (k2 % z_dev).astype(jnp.float32) + fz * z_dev
    back_mat = jnp.where(keep2, hat(slice_position(z2, dr_all, nz_all), row2), 0.0)

    total = part_ref[pl.ds(pl.multiple_of(me * cols, 8), cols), :]
    for k in range(n - 1):
        first[k].wait_recv()
        total = total + got[k]
    sums[...] = total
    for side, there, other in sides:

        @pl.when(there)
        def _():
            side_copy(sums, nbr, side, other, sb, rb).start()

    proj = jnp.dot(total, mats[2], precision=HI, preferred_element_type=jnp.float32)
    rays = ray_rows * jnp.dot(total, pick, precision=HI, preferred_element_type=jnp.float32)
    inverse = jnp.maximum(rays, 1.0)
    lc = lax.broadcasted_iota(jnp.int32, (cols, wide), 1)
    rc_row, _, rc_ok = row_of(lc)
    meas = meas_ref[...]

    for side, there, other in sides:

        @pl.when(there)
        def _():
            side_wait(meas_ref, mnbr, side, other, sm_sem, rm_sem)
            side_wait(sums, nbr, side, other, sb, rb)

        @pl.when(jnp.logical_not(there))
        def _():
            mnbr[side] = jnp.zeros_like(meas)
            nbr[side] = jnp.zeros_like(total)

    for side in range(2):
        proj = proj + jnp.dot(nbr[side], mats[side], precision=HI, preferred_element_type=jnp.float32)
    low = pltpu.roll(mnbr[0], wide - rows_dev, 1)
    high = pltpu.roll(mnbr[1], rows_dev, 1)
    meas = jnp.where(rc_row < margin, low, jnp.where(rc_row < margin + rows_dev, meas, high))
    residual = jnp.where(rc_ok, meas - proj / inverse, 0.0)
    res_ref[...] = residual
    rounded = residual.astype(jnp.bfloat16).astype(jnp.float32)
    smeared = jnp.dot(rounded, back_mat, precision=HI, preferred_element_type=jnp.float32)
    smeared = smeared.astype(jnp.bfloat16)
    own[...] = smeared
    mine = pl.ds(pl.multiple_of(me * cols, 16), cols)
    second = []
    for k, p in enumerate(peers):
        copy = pltpu.make_async_remote_copy(
            src_ref=own,
            dst_ref=sm_ref.at[mine],
            send_sem=sc.at[k],
            recv_sem=rc.at[k],
            device_id=(gz, p),
            device_id_type=MESH,
        )
        copy.start()
        second.append(copy)
    sm_ref[mine, :] = smeared
    for copy in first:
        copy.wait_send()
    for copy in second:
        copy.wait()


def local(ngz, n, volume, measured, view_order):
    z_dev, x_dev, ny = volume.shape
    rows_dev, cols = measured.shape[2:]
    nx_all, dc_all = x_dev * n, cols * n
    nz_all, dr_all = z_dev * ngz, rows_dev * ngz
    margin = nz_all // 40 + 3
    tiles = (x_dev // TX) * (ny // TY)
    count = VIEWS * SUBSETS
    gz, me = lax.axis_index("gz"), lax.axis_index("xy")
    cfg = (nx_all, ny, dc_all, x_dev)
    f32 = jnp.float32

    angles = 2.0 * math.pi * view_order[:count].astype(f32) / ANGLES
    cosine, sine = jnp.cos(angles), jnp.sin(angles)
    x_first = (me * x_dev).astype(f32)
    geom = jnp.concatenate(
        [cosine, sine, x_first[None], (gz * z_dev).astype(f32)[None]]
    )
    ids = jnp.arange(tiles, dtype=jnp.int32)
    tx = ((ids // (ny // TY)) * TX).astype(f32) + x_first
    ty = ((ids % (ny // TY)) * TY).astype(f32)
    lowest = None
    for dx in (0, TX - 1):
        for dy in (0, TY - 1):
            u = column_position(
                tx[None] + dx, ty[None] + dy, cosine[:, None], sine[:, None], nx_all, ny, dc_all
            )
            lowest = u if lowest is None else jnp.minimum(lowest, u)
    starts = jnp.clip(jnp.floor((lowest - 0.01) / STEP), 0, (dc_all - WIN) // STEP)
    starts = starts.astype(jnp.int32) * STEP

    meas_t = jnp.pad(
        measured.transpose(0, 3, 1, 2),
        ((0, 0), (0, 0), (0, 0), (margin, VROWS - margin - rows_dev)),
    ).reshape(SUBSETS, cols, VIEWS * VROWS)
    meas_t = jnp.pad(meas_t, ((0, 0), (0, 0), (0, 2 * LANES - VIEWS * VROWS)))

    smem = pl.BlockSpec(memory_space=pltpu.SMEM)
    vmem = pl.BlockSpec(memory_space=pltpu.VMEM)
    u_scr = pltpu.VMEM((VIEWS, tiles, LANES), f32)
    accs = [pltpu.VMEM((dc_all, LANES), f32) for _ in range(VIEWS)]
    tile_shape = jax.ShapeDtypeStruct((tiles, z_dev, LANES), f32)
    part_shape = jax.ShapeDtypeStruct((dc_all, LANES), f32)
    blocks = pltpu.VMEM(((dc_all - WIN) // STEP + 1, VIEWS, z_dev, LANES), jnp.bfloat16)

    tiled, part = pl.pallas_call(
        functools.partial(forward_kernel, cfg),
        out_shape=(tile_shape, part_shape),
        in_specs=[smem, smem, vmem],
        out_specs=(vmem, vmem),
        scratch_shapes=[u_scr, *accs],
    )(starts, geom, volume.reshape(z_dev * x_dev, ny))

    for subset in range(SUBSETS):
        last = subset == SUBSETS - 1
        dims = (n, ngz, z_dev, rows_dev, cols, margin)
        dma = pltpu.SemaphoreType.DMA
        smeared, residual = pl.pallas_call(
            functools.partial(comm_kernel, dims),
            out_shape=(
                jax.ShapeDtypeStruct((dc_all, LANES), jnp.bfloat16),
                jax.ShapeDtypeStruct((cols, 2 * LANES), f32),
            ),
            in_specs=[vmem, vmem],
            out_specs=(vmem, vmem),
            scratch_shapes=[
                pltpu.VMEM((n - 1, cols, LANES), f32),
                pltpu.VMEM((cols, LANES), f32),
                pltpu.VMEM((2, cols, LANES), f32),
                pltpu.VMEM((2, cols, 2 * LANES), f32),
                pltpu.VMEM((cols, LANES), jnp.bfloat16),
                dma((n - 1,)),
                dma((n - 1,)),
                dma((2,)),
                dma((2,)),
                dma((2,)),
                dma((2,)),
                dma((n - 1,)),
                dma((n - 1,)),
            ],
            compiler_params=pltpu.CompilerParams(collective_id=subset, has_side_effects=True),
        )(part, meas_t[subset])
        body = functools.partial(back_kernel, cfg, (dr_all, nz_all), subset)
        if last:
            volume_out = pl.pallas_call(
                body,
                out_shape=jax.ShapeDtypeStruct((z_dev * x_dev, ny), f32),
                in_specs=[smem, smem, vmem, vmem],
                out_specs=vmem,
                scratch_shapes=[u_scr, blocks, pltpu.VMEM(tile_shape.shape, f32)],
            )(starts, geom, tiled, smeared)
        else:
            tiled, part = pl.pallas_call(
                body,
                out_shape=(tile_shape, part_shape),
                in_specs=[smem, smem, vmem, vmem],
                out_specs=(vmem, vmem),
                scratch_shapes=[u_scr, blocks, u_scr, *accs],
            )(starts, geom, tiled, smeared)
    residual = residual[:, : VIEWS * VROWS].reshape(cols, VIEWS, VROWS)
    residual = residual[:, :, margin : margin + rows_dev].transpose(1, 2, 0)
    return (volume_out.reshape(z_dev, x_dev, ny), residual)


def solution(mesh):
    in_specs = (P("gz", "xy", None), P(None, None, "gz", "xy"), P())
    out_specs = (P("gz", "xy", None), P(None, "gz", "xy"))
    body = functools.partial(local, mesh.shape["gz"], mesh.shape["xy"])
    return jax.shard_map(body, mesh=mesh, in_specs=in_specs, out_specs=out_specs, check_vma=False)
```

```python
import functools
import math

import jax
import jax.numpy as jnp
from jax import lax
from jax.experimental import pallas as pl
from jax.experimental.pallas import tpu as pltpu
from jax.sharding import PartitionSpec as P

VIEWS = 5
SUBSETS = 2
ANGLES = 48
TX = 8
TY = 16
WIN = 48
STEP = 16
LANES = 128
GROUP = 4
VROWS = 32
HI = lax.Precision.HIGHEST
MESH = pl.DeviceIdType.MESH
NT = (((1,), (1,)), ((), ()))


def hat(pos, rows):
    return jnp.maximum(0.0, 1.0 - jnp.abs(pos - rows) / 2.0)


def slice_position(z, dr_all, nz_all):
    return (dr_all - 1) / 2.0 + 0.96 * (dr_all / nz_all) * (z - (nz_all - 1) / 2.0)


def column_position(x, y, cosine, sine, nx_all, ny, dc_all):
    xc = x - (nx_all - 1) / 2.0
    yc = y - (ny - 1) / 2.0
    along = xc * cosine + yc * sine
    depth = yc * cosine - xc * sine
    source = 2.0 * nx_all
    return (dc_all - 1) / 2.0 + 0.9 * (dc_all / nx_all) * along * source / (source + depth)


def tile_swap(rows):
    lane = lax.broadcasted_iota(jnp.int32, rows[0].shape, 1)
    for bit in (1, 2, 4):
        high = ((lane // TY) & bit) != 0
        new = []
        for i in range(TX):
            if i & bit:
                new.append(jnp.where(high, rows[i], pltpu.roll(rows[i - bit], LANES - TY * bit, 1)))
            else:
                new.append(jnp.where(high, pltpu.roll(rows[i + bit], TY * bit, 1), rows[i]))
        rows = new
    return rows


def fill_positions(u_ref, geom_ref, subset, cfg):
    nx_all, ny, dc_all, x_dev = cfg
    tiles = u_ref.shape[1]
    tile = lax.broadcasted_iota(jnp.int32, (tiles, LANES), 0)
    lane = lax.broadcasted_iota(jnp.int32, (tiles, LANES), 1)
    per = ny // TY
    x = ((tile // per) * TX + lane // TY).astype(jnp.float32) + geom_ref[2 * VIEWS * SUBSETS]
    y = ((tile % per) * TY + lane % TY).astype(jnp.float32)
    for v in range(VIEWS):
        k = subset * VIEWS + v
        u_ref[v] = column_position(
            x, y, geom_ref[k], geom_ref[VIEWS * SUBSETS + k], nx_all, ny, dc_all
        )


def weights_for(u_ref, v, t, start):
    row = u_ref[v, pl.ds(t, 1), :] - start.astype(jnp.float32)
    col = lax.broadcasted_iota(jnp.int32, (WIN, LANES), 0).astype(jnp.float32)
    return jnp.maximum(0.0, 1.0 - jnp.abs(row - col)).astype(jnp.bfloat16)


def project_tiles(group, first, subset, starts_ref, u_ref, accs):
    z_dev = group[0].shape[0]
    parts = [
        project_tile(tile, first + i, subset, starts_ref, u_ref) for i, tile in enumerate(group)
    ]
    for starts, part in parts:
        for v in range(VIEWS):
            where = pl.ds(starts[v], WIN)
            accs[v][where, : 2 * z_dev] += part[v * WIN : (v + 1) * WIN]


def project_tile(tile, t, subset, starts_ref, u_ref):
    z_dev = tile.shape[0]
    ones = jnp.where(
        lax.broadcasted_iota(jnp.int32, (z_dev, LANES), 0) == 0, 1.0, 0.0
    ).astype(jnp.bfloat16)
    a = jnp.concatenate([tile.astype(jnp.bfloat16), ones], axis=0)
    starts = [pl.multiple_of(starts_ref[subset * VIEWS + v, t], STEP) for v in range(VIEWS)]
    w = jnp.concatenate([weights_for(u_ref, v, t, starts[v]) for v in range(VIEWS)], axis=0)
    return starts, lax.dot_general(w, a, NT, preferred_element_type=jnp.float32)


def clear(accs):
    for acc in accs:
        acc[...] = jnp.zeros_like(acc)


def combine(accs, part_ref, z_dev):
    total = jnp.zeros(part_ref.shape, jnp.float32)
    lane = lax.broadcasted_iota(jnp.int32, part_ref.shape, 1)
    for v in range(VIEWS):
        a = accs[v][...]
        s = jnp.where(lane < z_dev, a, 0.0)
        n = jnp.where(lane == z_dev, a, 0.0)
        total = total + (pltpu.roll(s, z_dev * v, 1) if v else s)
        total = total + pltpu.roll(n, z_dev * (VIEWS - 1) + v, 1)
    part_ref[...] = total


def forward_kernel(cfg, starts_ref, geom_ref, vol_ref, tiles_ref, part_ref, u_ref, *accs):
    nx_all, ny, dc_all, x_dev = cfg
    tiles, z_dev = tiles_ref.shape[:2]
    fill_positions(u_ref, geom_ref, 0, cfg)
    clear(accs)
    per = ny // TY
    for g in range(x_dev // TX):
        rows = [vol_ref[pl.ds(g * TX + i, z_dev, stride=x_dev), :] for i in range(TX)]
        rows = tile_swap(rows)
        for j in range(per):
            tiles_ref[g * per + j] = rows[j]

    @pl.loop(0, tiles // GROUP)
    def _(step):
        first = step * GROUP
        group = [tiles_ref[first + i] for i in range(GROUP)]
        project_tiles(group, first, 0, starts_ref, u_ref, accs)

    combine(accs, part_ref, z_dev)


def make_blocks(sm_ref, blk_ref, z_dev):
    k = sm_ref.shape[1]
    eye = (
        lax.broadcasted_iota(jnp.int32, (k, k), 0) == lax.broadcasted_iota(jnp.int32, (k, k), 1)
    ).astype(jnp.bfloat16)
    rows = lax.dot_general(eye, sm_ref[...], NT, preferred_element_type=jnp.float32)
    for s in range(blk_ref.shape[0]):
        cut = rows[: VIEWS * z_dev, s * STEP : s * STEP + WIN].astype(jnp.bfloat16)
        for v in range(VIEWS):
            blk_ref[s, v, :, :WIN] = cut[v * z_dev : (v + 1) * z_dev]


def back_tile(tile, t, subset, starts_ref, u_ref, blk_ref, slice_total):
    z_dev = tile.shape[0]
    ones = jnp.where(
        lax.broadcasted_iota(jnp.int32, (z_dev, WIN), 0) == 0, 1.0, 0.0
    ).astype(jnp.bfloat16)
    total = jnp.zeros((2 * z_dev, LANES), jnp.float32)
    for v in range(VIEWS):
        start = starts_ref[subset * VIEWS + v, t]
        w = weights_for(u_ref, v, t, start)
        a = jnp.concatenate([blk_ref[start // STEP, v][:, :WIN], ones], axis=0)
        total = total + jnp.dot(a, w, preferred_element_type=jnp.float32)
    norm = slice_total * total[z_dev : z_dev + 1]
    return tile + total[:z_dev] / jnp.maximum(norm, 1.0)


def slice_totals(geom_ref, z_dev, dr_all, nz_all):
    z = lax.broadcasted_iota(jnp.int32, (z_dev, LANES), 0).astype(jnp.float32)
    pos = slice_position(z + geom_ref[2 * VIEWS * SUBSETS + 1], dr_all, nz_all)
    total = jnp.zeros((z_dev, LANES), jnp.float32)
    for r in range(dr_all):
        total = total + hat(pos, float(r))
    return total


def back_kernel(cfg, rows_cfg, subset, starts_ref, geom_ref, tiles_ref, sm_ref, *rest):
    nx_all, ny, dc_all, x_dev = cfg
    dr_all, nz_all = rows_cfg
    tiles, z_dev = tiles_ref.shape[:2]
    last = subset == SUBSETS - 1
    if last:
        vol_ref, u_ref, blk_ref, new_ref = rest
    else:
        new_ref, part_ref, u_ref, blk_ref, u2_ref, *accs = rest
        fill_positions(u2_ref, geom_ref, subset + 1, cfg)
        clear(accs)
    fill_positions(u_ref, geom_ref, subset, cfg)
    make_blocks(sm_ref, blk_ref, z_dev)
    slice_total = slice_totals(geom_ref, z_dev, dr_all, nz_all)

    @pl.loop(0, tiles // GROUP)
    def _(step):
        first = step * GROUP
        group = [
            back_tile(
                tiles_ref[first + i], first + i, subset, starts_ref, u_ref, blk_ref, slice_total
            )
            for i in range(GROUP)
        ]
        for i, tile in enumerate(group):
            new_ref[first + i] = tile
        if not last:
            project_tiles(group, first, subset + 1, starts_ref, u2_ref, accs)

    if not last:
        combine(accs, part_ref, z_dev)
        return
    per = ny // TY
    for g in range(x_dev // TX):
        rows = tile_swap([new_ref[g * per + j] for j in range(per)])
        for i in range(TX):
            vol_ref[pl.ds(g * TX + i, z_dev, stride=x_dev), :] = rows[i]


def comm_kernel(dims, part_ref, meas_ref, sm_ref, *rest):
    n, ngz, z_dev, rows_dev, cols, margin = dims
    (res_ref, got, sums, nbr, mnbr, own, sa, ra, sb, rb, sm_sem, rm_sem, sc, rc) = rest
    nz_all, dr_all = z_dev * ngz, rows_dev * ngz
    gz, me = lax.axis_index("gz"), lax.axis_index("xy")
    peers = [lax.rem(me + k, n) for k in range(1, n)]
    sides = ((0, gz > 0, gz - 1), (1, gz < ngz - 1, gz + 1))

    barrier = pltpu.get_barrier_semaphore()
    for p in peers:
        pl.semaphore_signal(barrier, inc=1, device_id=(gz, p), device_id_type=MESH)
    for _, there, other in sides:

        @pl.when(there)
        def _():
            pl.semaphore_signal(barrier, inc=1, device_id=(other, me), device_id_type=MESH)

    near = lax.div(gz + ngz - 1, ngz) + lax.div(2 * ngz - 2 - gz, ngz)
    pl.semaphore_wait(barrier, n - 1 + near)

    first = []
    for k, p in enumerate(peers):
        copy = pltpu.make_async_remote_copy(
            src_ref=part_ref.at[pl.ds(pl.multiple_of(p * cols, 8), cols)],
            dst_ref=got.at[k],
            send_sem=sa.at[k],
            recv_sem=ra.at[k],
            device_id=(gz, p),
            device_id_type=MESH,
        )
        copy.start()
        first.append(copy)

    def side_copy(src, dst, side, other, send, recv):
        return pltpu.make_async_remote_copy(
            src_ref=src,
            dst_ref=dst.at[1 - side],
            send_sem=send.at[side],
            recv_sem=recv.at[1 - side],
            device_id=(other, me),
            device_id_type=MESH,
        )

    def side_wait(src, dst, side, other, send, recv):
        side_copy(src, dst, side, other, send, recv).wait_send()
        side_copy(src, dst, 1 - side, other, send, recv).wait_recv()

    for side, there, other in sides:

        @pl.when(there)
        def _():
            side_copy(meas_ref, mnbr, side, other, sm_sem, rm_sem).start()

    wide = 2 * LANES
    fz = gz.astype(jnp.float32)
    kk = lax.broadcasted_iota(jnp.int32, (LANES, wide), 0)
    ll = lax.broadcasted_iota(jnp.int32, (LANES, wide), 1)
    same = jnp.logical_and(kk // z_dev == ll // VROWS, kk < VIEWS * z_dev)
    ext = rows_dev + 2 * margin

    def row_of(lanes):
        rr = lanes % VROWS
        row = (rr - margin).astype(jnp.float32) + fz * rows_dev
        ok = (rr < ext) & (row >= 0) & (row < dr_all) & (lanes < VIEWS * VROWS)
        return rr, row, ok

    rr, row, ok = row_of(ll)
    keep = jnp.logical_and(same, ok)
    zz = (kk % z_dev).astype(jnp.float32)

    def slab(shift):
        z = zz + (fz + shift) * z_dev
        return jnp.where(keep, hat(slice_position(z, dr_all, nz_all), row), 0.0)

    mats = [slab(-1), slab(1), slab(0)]
    pick = (kk == VIEWS * z_dev + ll // VROWS).astype(jnp.float32)
    z_all = lax.broadcasted_iota(jnp.int32, (nz_all, wide), 0).astype(jnp.float32)
    _, row_all, _ = row_of(lax.broadcasted_iota(jnp.int32, (nz_all, wide), 1))
    ray_rows = jnp.sum(
        hat(slice_position(z_all, dr_all, nz_all), row_all), axis=0, keepdims=True
    )
    l2 = lax.broadcasted_iota(jnp.int32, (wide, LANES), 0)
    k2 = lax.broadcasted_iota(jnp.int32, (wide, LANES), 1)
    _, row2, ok2 = row_of(l2)
    keep2 = ok2 & (k2 // z_dev == l2 // VROWS) & (k2 < VIEWS * z_dev)
    z2 = (k2 % z_dev).astype(jnp.float32) + fz * z_dev
    back_mat = jnp.where(keep2, hat(slice_position(z2, dr_all, nz_all), row2), 0.0)

    total = part_ref[pl.ds(pl.multiple_of(me * cols, 8), cols), :]
    for k in range(n - 1):
        first[k].wait_recv()
        total = total + got[k]
    sums[...] = total
    for side, there, other in sides:

        @pl.when(there)
        def _():
            side_copy(sums, nbr, side, other, sb, rb).start()

    proj = jnp.dot(total, mats[2], precision=HI, preferred_element_type=jnp.float32)
    rays = ray_rows * jnp.dot(total, pick, precision=HI, preferred_element_type=jnp.float32)
    inverse = jnp.maximum(rays, 1.0)
    lc = lax.broadcasted_iota(jnp.int32, (cols, wide), 1)
    rc_row, _, rc_ok = row_of(lc)
    meas = meas_ref[...]

    for side, there, other in sides:

        @pl.when(there)
        def _():
            side_wait(meas_ref, mnbr, side, other, sm_sem, rm_sem)
            side_wait(sums, nbr, side, other, sb, rb)

        @pl.when(jnp.logical_not(there))
        def _():
            mnbr[side] = jnp.zeros_like(meas)
            nbr[side] = jnp.zeros_like(total)

    for side in range(2):
        proj = proj + jnp.dot(nbr[side], mats[side], precision=HI, preferred_element_type=jnp.float32)
    low = pltpu.roll(mnbr[0], wide - rows_dev, 1)
    high = pltpu.roll(mnbr[1], rows_dev, 1)
    meas = jnp.where(rc_row < margin, low, jnp.where(rc_row < margin + rows_dev, meas, high))
    residual = jnp.where(rc_ok, meas - proj / inverse, 0.0)
    res_ref[...] = residual
    rounded = residual.astype(jnp.bfloat16).astype(jnp.float32)
    smeared = jnp.dot(rounded, back_mat, precision=HI, preferred_element_type=jnp.float32)
    smeared = smeared.astype(jnp.bfloat16)
    own[...] = smeared
    mine = pl.ds(pl.multiple_of(me * cols, 16), cols)
    second = []
    for k, p in enumerate(peers):
        copy = pltpu.make_async_remote_copy(
            src_ref=own,
            dst_ref=sm_ref.at[mine],
            send_sem=sc.at[k],
            recv_sem=rc.at[k],
            device_id=(gz, p),
            device_id_type=MESH,
        )
        copy.start()
        second.append(copy)
    sm_ref[mine, :] = smeared
    for copy in first:
        copy.wait_send()
    for copy in second:
        copy.wait()


def local(ngz, n, volume, measured, view_order):
    z_dev, x_dev, ny = volume.shape
    rows_dev, cols = measured.shape[2:]
    nx_all, dc_all = x_dev * n, cols * n
    nz_all, dr_all = z_dev * ngz, rows_dev * ngz
    margin = nz_all // 40 + 3
    tiles = (x_dev // TX) * (ny // TY)
    count = VIEWS * SUBSETS
    gz, me = lax.axis_index("gz"), lax.axis_index("xy")
    cfg = (nx_all, ny, dc_all, x_dev)
    f32 = jnp.float32

    angles = 2.0 * math.pi * view_order[:count].astype(f32) / ANGLES
    cosine, sine = jnp.cos(angles), jnp.sin(angles)
    x_first = (me * x_dev).astype(f32)
    geom = jnp.concatenate(
        [cosine, sine, x_first[None], (gz * z_dev).astype(f32)[None]]
    )
    ids = jnp.arange(tiles, dtype=jnp.int32)
    tx = ((ids // (ny // TY)) * TX).astype(f32) + x_first
    ty = ((ids % (ny // TY)) * TY).astype(f32)
    lowest = None
    for dx in (0, TX - 1):
        for dy in (0, TY - 1):
            u = column_position(
                tx[None] + dx, ty[None] + dy, cosine[:, None], sine[:, None], nx_all, ny, dc_all
            )
            lowest = u if lowest is None else jnp.minimum(lowest, u)
    starts = jnp.clip(jnp.floor((lowest - 0.01) / STEP), 0, (dc_all - WIN) // STEP)
    starts = starts.astype(jnp.int32) * STEP

    meas_t = jnp.pad(
        measured.transpose(0, 3, 1, 2),
        ((0, 0), (0, 0), (0, 0), (margin, VROWS - margin - rows_dev)),
    ).reshape(SUBSETS, cols, VIEWS * VROWS)
    meas_t = jnp.pad(meas_t, ((0, 0), (0, 0), (0, 2 * LANES - VIEWS * VROWS)))

    smem = pl.BlockSpec(memory_space=pltpu.SMEM)
    vmem = pl.BlockSpec(memory_space=pltpu.VMEM)
    u_scr = pltpu.VMEM((VIEWS, tiles, LANES), f32)
    accs = [pltpu.VMEM((dc_all, LANES), f32) for _ in range(VIEWS)]
    tile_shape = jax.ShapeDtypeStruct((tiles, z_dev, LANES), f32)
    part_shape = jax.ShapeDtypeStruct((dc_all, LANES), f32)
    blocks = pltpu.VMEM(((dc_all - WIN) // STEP + 1, VIEWS, z_dev, LANES), jnp.bfloat16)

    tiled, part = pl.pallas_call(
        functools.partial(forward_kernel, cfg),
        out_shape=(tile_shape, part_shape),
        in_specs=[smem, smem, vmem],
        out_specs=(vmem, vmem),
        scratch_shapes=[u_scr, *accs],
    )(starts, geom, volume.reshape(z_dev * x_dev, ny))

    for subset in range(SUBSETS):
        last = subset == SUBSETS - 1
        dims = (n, ngz, z_dev, rows_dev, cols, margin)
        dma = pltpu.SemaphoreType.DMA
        smeared, residual = pl.pallas_call(
            functools.partial(comm_kernel, dims),
            out_shape=(
                jax.ShapeDtypeStruct((dc_all, LANES), jnp.bfloat16),
                jax.ShapeDtypeStruct((cols, 2 * LANES), f32),
            ),
            in_specs=[vmem, vmem],
            out_specs=(vmem, vmem),
            scratch_shapes=[
                pltpu.VMEM((n - 1, cols, LANES), f32),
                pltpu.VMEM((cols, LANES), f32),
                pltpu.VMEM((2, cols, LANES), f32),
                pltpu.VMEM((2, cols, 2 * LANES), f32),
                pltpu.VMEM((cols, LANES), jnp.bfloat16),
                dma((n - 1,)),
                dma((n - 1,)),
                dma((2,)),
                dma((2,)),
                dma((2,)),
                dma((2,)),
                dma((n - 1,)),
                dma((n - 1,)),
            ],
            compiler_params=pltpu.CompilerParams(collective_id=subset, has_side_effects=True),
        )(part, meas_t[subset])
        body = functools.partial(back_kernel, cfg, (dr_all, nz_all), subset)
        if last:
            volume_out = pl.pallas_call(
                body,
                out_shape=jax.ShapeDtypeStruct((z_dev * x_dev, ny), f32),
                in_specs=[smem, smem, vmem, vmem],
                out_specs=vmem,
                scratch_shapes=[u_scr, blocks, pltpu.VMEM(tile_shape.shape, f32)],
            )(starts, geom, tiled, smeared)
        else:
            tiled, part = pl.pallas_call(
                body,
                out_shape=(tile_shape, part_shape),
                in_specs=[smem, smem, vmem, vmem],
                out_specs=(vmem, vmem),
                scratch_shapes=[u_scr, blocks, u_scr, *accs],
            )(starts, geom, tiled, smeared)
    residual = residual[:, : VIEWS * VROWS].reshape(cols, VIEWS, VROWS)
    residual = residual[:, :, margin : margin + rows_dev].transpose(1, 2, 0)
    return (volume_out.reshape(z_dev, x_dev, ny), residual)


def solution(mesh):
    in_specs = (P("gz", "xy", None), P(None, None, "gz", "xy"), P())
    out_specs = (P("gz", "xy", None), P(None, "gz", "xy"))
    body = functools.partial(local, mesh.shape["gz"], mesh.shape["xy"])
    return jax.shard_map(body, mesh=mesh, in_specs=in_specs, out_specs=out_specs, check_vma=False)
```

```python
import functools
import math

import jax
import jax.numpy as jnp
from jax import lax
from jax.experimental import pallas as pl
from jax.experimental.pallas import tpu as pltpu
from jax.sharding import PartitionSpec as P

VIEWS = 5
SUBSETS = 2
ANGLES = 48
TX = 8
TY = 16
WIN = 48
STEP = 16
LANES = 128
GROUP = 8
VROWS = 32
MESH = pl.DeviceIdType.MESH
NT = (((1,), (1,)), ((), ()))


def hat(pos, rows):
    return jnp.maximum(0.0, 1.0 - jnp.abs(pos - rows) / 2.0)


def slice_position(z, dr_all, nz_all):
    return (dr_all - 1) / 2.0 + 0.96 * (dr_all / nz_all) * (z - (nz_all - 1) / 2.0)


def column_position(x, y, cosine, sine, nx_all, ny, dc_all):
    xc = x - (nx_all - 1) / 2.0
    yc = y - (ny - 1) / 2.0
    along = xc * cosine + yc * sine
    depth = yc * cosine - xc * sine
    source = 2.0 * nx_all
    return (dc_all - 1) / 2.0 + 0.9 * (dc_all / nx_all) * along * source / (source + depth)


def tile_swap(rows):
    lane = lax.broadcasted_iota(jnp.int32, rows[0].shape, 1)
    for bit in (1, 2, 4):
        high = ((lane // TY) & bit) != 0
        new = []
        for i in range(TX):
            if i & bit:
                new.append(jnp.where(high, rows[i], pltpu.roll(rows[i - bit], LANES - TY * bit, 1)))
            else:
                new.append(jnp.where(high, pltpu.roll(rows[i + bit], TY * bit, 1), rows[i]))
        rows = new
    return rows


def fill_positions(u_ref, geom_ref, subset, cfg):
    nx_all, ny, dc_all, x_dev = cfg
    tiles = u_ref.shape[1]
    tile = lax.broadcasted_iota(jnp.int32, (tiles, LANES), 0)
    lane = lax.broadcasted_iota(jnp.int32, (tiles, LANES), 1)
    per = ny // TY
    x = ((tile // per) * TX + lane // TY).astype(jnp.float32) + geom_ref[2 * VIEWS * SUBSETS]
    y = ((tile % per) * TY + lane % TY).astype(jnp.float32)
    for v in range(VIEWS):
        k = subset * VIEWS + v
        u_ref[v] = column_position(
            x, y, geom_ref[k], geom_ref[VIEWS * SUBSETS + k], nx_all, ny, dc_all
        )


def weights_for(u_ref, v, t, start):
    row = u_ref[v, pl.ds(t, 1), :] - start.astype(jnp.float32)
    col = lax.broadcasted_iota(jnp.int32, (WIN, LANES), 0).astype(jnp.float32)
    return jnp.maximum(0.0, 1.0 - jnp.abs(row - col)).astype(jnp.bfloat16)


def project_tiles(group, first, subset, starts_ref, u_ref, accs):
    z_dev = group[0].shape[0]
    parts = [
        project_tile(tile, first + i, subset, starts_ref, u_ref) for i, tile in enumerate(group)
    ]
    for starts, part in parts:
        for v in range(VIEWS):
            where = pl.ds(starts[v], WIN)
            accs[v][where, : 2 * z_dev] += part[v * WIN : (v + 1) * WIN]


def project_tile(tile, t, subset, starts_ref, u_ref):
    z_dev = tile.shape[0]
    ones = jnp.where(
        lax.broadcasted_iota(jnp.int32, (z_dev, LANES), 0) == 0, 1.0, 0.0
    ).astype(jnp.bfloat16)
    a = jnp.concatenate([tile.astype(jnp.bfloat16), ones], axis=0)
    starts = [pl.multiple_of(starts_ref[subset * VIEWS + v, t], STEP) for v in range(VIEWS)]
    w = jnp.concatenate([weights_for(u_ref, v, t, starts[v]) for v in range(VIEWS)], axis=0)
    return starts, lax.dot_general(w, a, NT, preferred_element_type=jnp.float32)


def clear(accs):
    for acc in accs:
        acc[...] = jnp.zeros_like(acc)


def combine(accs, part_ref, z_dev):
    total = jnp.zeros(part_ref.shape, jnp.float32)
    lane = lax.broadcasted_iota(jnp.int32, part_ref.shape, 1)
    for v in range(VIEWS):
        a = accs[v][...]
        s = jnp.where(lane < z_dev, a, 0.0)
        n = jnp.where(lane == z_dev, a, 0.0)
        total = total + (pltpu.roll(s, z_dev * v, 1) if v else s)
        total = total + pltpu.roll(n, z_dev * (VIEWS - 1) + v, 1)
    part_ref[...] = total


def forward_kernel(cfg, starts_ref, geom_ref, vol_ref, tiles_ref, part_ref, u_ref, *accs):
    nx_all, ny, dc_all, x_dev = cfg
    tiles, z_dev = tiles_ref.shape[:2]
    fill_positions(u_ref, geom_ref, 0, cfg)
    clear(accs)
    per = ny // TY
    for g in range(x_dev // TX):
        rows = [vol_ref[pl.ds(g * TX + i, z_dev, stride=x_dev), :] for i in range(TX)]
        rows = tile_swap(rows)
        for j in range(per):
            tiles_ref[g * per + j] = rows[j]

    @pl.loop(0, tiles // GROUP)
    def _(step):
        first = step * GROUP
        group = [tiles_ref[first + i] for i in range(GROUP)]
        project_tiles(group, first, 0, starts_ref, u_ref, accs)

    combine(accs, part_ref, z_dev)


def make_blocks(sm_ref, blk_ref, z_dev):
    k = sm_ref.shape[1]
    eye = (
        lax.broadcasted_iota(jnp.int32, (k, k), 0) == lax.broadcasted_iota(jnp.int32, (k, k), 1)
    ).astype(jnp.bfloat16)
    rows = lax.dot_general(eye, sm_ref[...], NT, preferred_element_type=jnp.float32)
    for s in range(blk_ref.shape[0]):
        cut = rows[: VIEWS * z_dev, s * STEP : s * STEP + WIN].astype(jnp.bfloat16)
        for v in range(VIEWS):
            blk_ref[s, v, :, :WIN] = cut[v * z_dev : (v + 1) * z_dev]


def back_tile(tile, t, subset, starts_ref, u_ref, blk_ref, slice_total):
    z_dev = tile.shape[0]
    ones = jnp.where(
        lax.broadcasted_iota(jnp.int32, (z_dev, WIN), 0) == 0, 1.0, 0.0
    ).astype(jnp.bfloat16)
    total = jnp.zeros((2 * z_dev, LANES), jnp.float32)
    for v in range(VIEWS):
        start = starts_ref[subset * VIEWS + v, t]
        w = weights_for(u_ref, v, t, start)
        a = jnp.concatenate([blk_ref[start // STEP, v][:, :WIN], ones], axis=0)
        total = total + jnp.dot(a, w, preferred_element_type=jnp.float32)
    norm = slice_total * total[z_dev : z_dev + 1]
    return tile + total[:z_dev] / jnp.maximum(norm, 1.0)


def slice_totals(geom_ref, z_dev, dr_all, nz_all):
    z = lax.broadcasted_iota(jnp.int32, (z_dev, LANES), 0).astype(jnp.float32)
    pos = slice_position(z + geom_ref[2 * VIEWS * SUBSETS + 1], dr_all, nz_all)
    total = jnp.zeros((z_dev, LANES), jnp.float32)
    for r in range(dr_all):
        total = total + hat(pos, float(r))
    return total


def back_kernel(cfg, rows_cfg, subset, starts_ref, geom_ref, tiles_ref, sm_ref, *rest):
    nx_all, ny, dc_all, x_dev = cfg
    dr_all, nz_all = rows_cfg
    tiles, z_dev = tiles_ref.shape[:2]
    last = subset == SUBSETS - 1
    if last:
        vol_ref, u_ref, blk_ref, new_ref = rest
    else:
        new_ref, part_ref, u_ref, blk_ref, u2_ref, *accs = rest
        fill_positions(u2_ref, geom_ref, subset + 1, cfg)
        clear(accs)
    fill_positions(u_ref, geom_ref, subset, cfg)
    make_blocks(sm_ref, blk_ref, z_dev)
    slice_total = slice_totals(geom_ref, z_dev, dr_all, nz_all)

    @pl.loop(0, tiles // GROUP)
    def _(step):
        first = step * GROUP
        group = [
            back_tile(
                tiles_ref[first + i], first + i, subset, starts_ref, u_ref, blk_ref, slice_total
            )
            for i in range(GROUP)
        ]
        for i, tile in enumerate(group):
            new_ref[first + i] = tile
        if not last:
            project_tiles(group, first, subset + 1, starts_ref, u2_ref, accs)

    if not last:
        combine(accs, part_ref, z_dev)
        return
    per = ny // TY
    for g in range(x_dev // TX):
        rows = tile_swap([new_ref[g * per + j] for j in range(per)])
        for i in range(TX):
            vol_ref[pl.ds(g * TX + i, z_dev, stride=x_dev), :] = rows[i]


def split3(x):
    a = x.astype(jnp.bfloat16)
    rest = x - a.astype(jnp.float32)
    b = rest.astype(jnp.bfloat16)
    return a, b, (rest - b.astype(jnp.float32)).astype(jnp.bfloat16)


def split_dot(terms, mats):
    m = terms[0].shape[0]
    one = jnp.dot(jnp.concatenate(terms, axis=0), mats[0], preferred_element_type=jnp.float32)
    two = jnp.dot(
        jnp.concatenate(terms[:2], axis=0), mats[1], preferred_element_type=jnp.float32
    )
    three = jnp.dot(terms[0], mats[2], preferred_element_type=jnp.float32)
    small = one[2 * m :] + two[m:] + three
    return one[:m] + ((one[m : 2 * m] + two[:m]) + small)


def comm_kernel(dims, part_ref, meas_ref, sm_ref, *rest):
    n, ngz, z_dev, rows_dev, cols, margin = dims
    (res_ref, got, sums, nbr, mnbr, own, sa, ra, sb, rb, sm_sem, rm_sem, sc, rc, slabs, backs) = rest
    nz_all, dr_all = z_dev * ngz, rows_dev * ngz
    gz, me = lax.axis_index("gz"), lax.axis_index("xy")
    peers = [lax.rem(me + k, n) for k in range(1, n)]
    sides = ((0, gz > 0, gz - 1), (1, gz < ngz - 1, gz + 1))

    barrier = pltpu.get_barrier_semaphore()
    for p in peers:
        pl.semaphore_signal(barrier, inc=1, device_id=(gz, p), device_id_type=MESH)
    for _, there, other in sides:

        @pl.when(there)
        def _():
            pl.semaphore_signal(barrier, inc=1, device_id=(other, me), device_id_type=MESH)

    near = lax.div(gz + ngz - 1, ngz) + lax.div(2 * ngz - 2 - gz, ngz)
    pl.semaphore_wait(barrier, n - 1 + near)

    first = []
    for k, p in enumerate(peers):
        copy = pltpu.make_async_remote_copy(
            src_ref=part_ref.at[pl.ds(pl.multiple_of(p * cols, 8), cols)],
            dst_ref=got.at[k],
            send_sem=sa.at[k],
            recv_sem=ra.at[k],
            device_id=(gz, p),
            device_id_type=MESH,
        )
        copy.start()
        first.append(copy)

    def side_copy(src, dst, side, other, send, recv):
        return pltpu.make_async_remote_copy(
            src_ref=src,
            dst_ref=dst.at[1 - side],
            send_sem=send.at[side],
            recv_sem=recv.at[1 - side],
            device_id=(other, me),
            device_id_type=MESH,
        )

    def side_wait(src, dst, side, other, send, recv):
        side_copy(src, dst, side, other, send, recv).wait_send()
        side_copy(src, dst, 1 - side, other, send, recv).wait_recv()

    for side, there, other in sides:

        @pl.when(there)
        def _():
            side_copy(meas_ref, mnbr, side, other, sm_sem, rm_sem).start()

    wide = 2 * LANES
    fz = gz.astype(jnp.float32)
    kk = lax.broadcasted_iota(jnp.int32, (LANES, wide), 0)
    ll = lax.broadcasted_iota(jnp.int32, (LANES, wide), 1)
    same = jnp.logical_and(kk // z_dev == ll // VROWS, kk < VIEWS * z_dev)
    ext = rows_dev + 2 * margin

    def row_of(lanes):
        rr = lanes % VROWS
        row = (rr - margin).astype(jnp.float32) + fz * rows_dev
        ok = (rr < ext) & (row >= 0) & (row < dr_all) & (lanes < VIEWS * VROWS)
        return rr, row, ok

    rr, row, ok = row_of(ll)
    keep = jnp.logical_and(same, ok)
    zz = (kk % z_dev).astype(jnp.float32)

    def slab(shift):
        z = zz + (fz + shift) * z_dev
        return jnp.where(keep, hat(slice_position(z, dr_all, nz_all), row), 0.0)

    for i, shift in enumerate((-1, 1, 0)):
        for j, term in enumerate(split3(slab(shift))):
            slabs[i, j] = term
    pick = jnp.where(kk == VIEWS * z_dev + ll // VROWS, 1.0, 0.0).astype(jnp.bfloat16)
    z_all = lax.broadcasted_iota(jnp.int32, (nz_all, wide), 0).astype(jnp.float32)
    _, row_all, _ = row_of(lax.broadcasted_iota(jnp.int32, (nz_all, wide), 1))
    ray_rows = jnp.sum(
        hat(slice_position(z_all, dr_all, nz_all), row_all), axis=0, keepdims=True
    )
    l2 = lax.broadcasted_iota(jnp.int32, (wide, LANES), 0)
    k2 = lax.broadcasted_iota(jnp.int32, (wide, LANES), 1)
    _, row2, ok2 = row_of(l2)
    keep2 = ok2 & (k2 // z_dev == l2 // VROWS) & (k2 < VIEWS * z_dev)
    z2 = (k2 % z_dev).astype(jnp.float32) + fz * z_dev
    back_mat = jnp.where(keep2, hat(slice_position(z2, dr_all, nz_all), row2), 0.0)
    for j, term in enumerate(split3(back_mat)):
        backs[j] = term

    total = part_ref[pl.ds(pl.multiple_of(me * cols, 8), cols), :]
    for k in range(n - 1):
        first[k].wait_recv()
        total = total + got[k]
    sums[...] = total
    for side, there, other in sides:

        @pl.when(there)
        def _():
            side_copy(sums, nbr, side, other, sb, rb).start()

    terms = split3(total)
    proj = split_dot(terms, [slabs[2, j] for j in range(3)])
    three = jnp.dot(jnp.concatenate(terms, axis=0), pick, preferred_element_type=jnp.float32)
    rays = ray_rows * (three[:cols] + (three[cols : 2 * cols] + three[2 * cols :]))
    inverse = jnp.maximum(rays, 1.0)
    lc = lax.broadcasted_iota(jnp.int32, (cols, wide), 1)
    rc_row, _, rc_ok = row_of(lc)
    meas = meas_ref[...]

    for side, there, other in sides:

        @pl.when(there)
        def _():
            side_wait(meas_ref, mnbr, side, other, sm_sem, rm_sem)
            side_wait(sums, nbr, side, other, sb, rb)

        @pl.when(jnp.logical_not(there))
        def _():
            mnbr[side] = jnp.zeros_like(meas)
            nbr[side] = jnp.zeros_like(total)

    for side in range(2):
        proj = proj + split_dot(split3(nbr[side]), [slabs[side, j] for j in range(3)])
    low = pltpu.roll(mnbr[0], wide - rows_dev, 1)
    high = pltpu.roll(mnbr[1], rows_dev, 1)
    meas = jnp.where(rc_row < margin, low, jnp.where(rc_row < margin + rows_dev, meas, high))
    residual = jnp.where(rc_ok, meas - proj / inverse, 0.0)
    res_ref[...] = residual
    rounded = residual.astype(jnp.bfloat16)
    pieces = [jnp.dot(rounded, backs[j], preferred_element_type=jnp.float32) for j in range(3)]
    smeared = (pieces[0] + (pieces[1] + pieces[2])).astype(jnp.bfloat16)
    own[...] = smeared
    mine = pl.ds(pl.multiple_of(me * cols, 16), cols)
    second = []
    for k, p in enumerate(peers):
        copy = pltpu.make_async_remote_copy(
            src_ref=own,
            dst_ref=sm_ref.at[mine],
            send_sem=sc.at[k],
            recv_sem=rc.at[k],
            device_id=(gz, p),
            device_id_type=MESH,
        )
        copy.start()
        second.append(copy)
    sm_ref[mine, :] = smeared
    for copy in first:
        copy.wait_send()
    for copy in second:
        copy.wait()


def local(ngz, n, volume, measured, view_order):
    z_dev, x_dev, ny = volume.shape
    rows_dev, cols = measured.shape[2:]
    nx_all, dc_all = x_dev * n, cols * n
    nz_all, dr_all = z_dev * ngz, rows_dev * ngz
    margin = nz_all // 40 + 3
    tiles = (x_dev // TX) * (ny // TY)
    count = VIEWS * SUBSETS
    gz, me = lax.axis_index("gz"), lax.axis_index("xy")
    cfg = (nx_all, ny, dc_all, x_dev)
    f32 = jnp.float32

    angles = 2.0 * math.pi * view_order[:count].astype(f32) / ANGLES
    cosine, sine = jnp.cos(angles), jnp.sin(angles)
    x_first = (me * x_dev).astype(f32)
    geom = jnp.concatenate(
        [cosine, sine, x_first[None], (gz * z_dev).astype(f32)[None]]
    )
    ids = jnp.arange(tiles, dtype=jnp.int32)
    tx = ((ids // (ny // TY)) * TX).astype(f32) + x_first
    ty = ((ids % (ny // TY)) * TY).astype(f32)
    lowest = None
    for dx in (0, TX - 1):
        for dy in (0, TY - 1):
            u = column_position(
                tx[None] + dx, ty[None] + dy, cosine[:, None], sine[:, None], nx_all, ny, dc_all
            )
            lowest = u if lowest is None else jnp.minimum(lowest, u)
    starts = jnp.clip(jnp.floor((lowest - 0.01) / STEP), 0, (dc_all - WIN) // STEP)
    starts = starts.astype(jnp.int32) * STEP

    meas_t = jnp.pad(
        measured.transpose(0, 3, 1, 2),
        ((0, 0), (0, 0), (0, 0), (margin, VROWS - margin - rows_dev)),
    ).reshape(SUBSETS, cols, VIEWS * VROWS)
    meas_t = jnp.pad(meas_t, ((0, 0), (0, 0), (0, 2 * LANES - VIEWS * VROWS)))

    smem = pl.BlockSpec(memory_space=pltpu.SMEM)
    vmem = pl.BlockSpec(memory_space=pltpu.VMEM)
    u_scr = pltpu.VMEM((VIEWS, tiles, LANES), f32)
    accs = [pltpu.VMEM((dc_all, LANES), f32) for _ in range(VIEWS)]
    tile_shape = jax.ShapeDtypeStruct((tiles, z_dev, LANES), f32)
    part_shape = jax.ShapeDtypeStruct((dc_all, LANES), f32)
    blocks = pltpu.VMEM(((dc_all - WIN) // STEP + 1, VIEWS, z_dev, LANES), jnp.bfloat16)

    tiled, part = pl.pallas_call(
        functools.partial(forward_kernel, cfg),
        out_shape=(tile_shape, part_shape),
        in_specs=[smem, smem, vmem],
        out_specs=(vmem, vmem),
        scratch_shapes=[u_scr, *accs],
    )(starts, geom, volume.reshape(z_dev * x_dev, ny))

    for subset in range(SUBSETS):
        last = subset == SUBSETS - 1
        dims = (n, ngz, z_dev, rows_dev, cols, margin)
        dma = pltpu.SemaphoreType.DMA
        smeared, residual = pl.pallas_call(
            functools.partial(comm_kernel, dims),
            out_shape=(
                jax.ShapeDtypeStruct((dc_all, LANES), jnp.bfloat16),
                jax.ShapeDtypeStruct((cols, 2 * LANES), f32),
            ),
            in_specs=[vmem, vmem],
            out_specs=(vmem, vmem),
            scratch_shapes=[
                pltpu.VMEM((n - 1, cols, LANES), f32),
                pltpu.VMEM((cols, LANES), f32),
                pltpu.VMEM((2, cols, LANES), f32),
                pltpu.VMEM((2, cols, 2 * LANES), f32),
                pltpu.VMEM((cols, LANES), jnp.bfloat16),
                dma((n - 1,)),
                dma((n - 1,)),
                dma((2,)),
                dma((2,)),
                dma((2,)),
                dma((2,)),
                dma((n - 1,)),
                dma((n - 1,)),
                pltpu.VMEM((3, 3, LANES, 2 * LANES), jnp.bfloat16),
                pltpu.VMEM((3, 2 * LANES, LANES), jnp.bfloat16),
            ],
            compiler_params=pltpu.CompilerParams(collective_id=subset, has_side_effects=True),
        )(part, meas_t[subset])
        body = functools.partial(back_kernel, cfg, (dr_all, nz_all), subset)
        if last:
            volume_out = pl.pallas_call(
                body,
                out_shape=jax.ShapeDtypeStruct((z_dev * x_dev, ny), f32),
                in_specs=[smem, smem, vmem, vmem],
                out_specs=vmem,
                scratch_shapes=[u_scr, blocks, pltpu.VMEM(tile_shape.shape, f32)],
            )(starts, geom, tiled, smeared)
        else:
            tiled, part = pl.pallas_call(
                body,
                out_shape=(tile_shape, part_shape),
                in_specs=[smem, smem, vmem, vmem],
                out_specs=(vmem, vmem),
                scratch_shapes=[u_scr, blocks, u_scr, *accs],
            )(starts, geom, tiled, smeared)
    residual = residual[:, : VIEWS * VROWS].reshape(cols, VIEWS, VROWS)
    residual = residual[:, :, margin : margin + rows_dev].transpose(1, 2, 0)
    return (volume_out.reshape(z_dev, x_dev, ny), residual)


def solution(mesh):
    in_specs = (P("gz", "xy", None), P(None, None, "gz", "xy"), P())
    out_specs = (P("gz", "xy", None), P(None, "gz", "xy"))
    body = functools.partial(local, mesh.shape["gz"], mesh.shape["xy"])
    return jax.shard_map(body, mesh=mesh, in_specs=in_specs, out_specs=out_specs, check_vma=False)
```
